256 devices in a mesh: row: 16 (over x, y_hi, core), col: 16 (over y_lo, z).
Axes of the slice: x: 4, y: 4 (y_hi: 2, y_lo: 2; y = y_hi * 2 + y_lo), z: 8, core: 2. Of those that a mesh axis runs over, the one named last changes fastest.
Arguments:
- points: bfloat16 [32768, 128], P(('row', 'col')), may hold values from -6 to 6
- abar: bfloat16 [32768, 16, 16, 128], P('row', None, 'col'), may hold values from -6 to 6
- inv_scale: float32 [128], replicated, may hold values from 0.05 to 0.2
Outputs:
- point_grad: float32 [32768, 128], P(('row', 'col'))
The draws below stay inside these ranges and needn't reach their ends.
All inputs are finite; a program needn't handle non-finite values.
Results may differ from the reference program's by a relative error of at most 0.0052.
Values may be sent and summed in bfloat16 or wider, within the bound.
A program may use at most 64 MiB of HBM per device.

```python
import math
import jax
import jax.numpy as jnp
from jax import lax

FEAT = 128
PTS = 128
NPTS = 32768
N_ROW = 16
N_COL = 16


def with_spikes(values, key, source, target, parts, factor):
    owner, partner = [(jnp.arange(values.shape[dim]) // (values.shape[dim] // parts)).reshape([-1 if axis == dim else 1 for axis in range(values.ndim)]) for dim in (source, target)]
    chosen = jax.random.permutation(key, parts)[partner]
    strong = (owner == chosen) | (owner == (partner + parts // 2) % parts)
    return jnp.where(strong, factor * values, values)


def level_of(own_key, shape, cuts, least, high):
    level, own = 1.0, jax.random.fold_in(own_key, 6)
    for axis_at, parts in cuts:
        heights = jnp.exp(jax.random.uniform(jax.random.fold_in(own, axis_at), (parts,), jnp.float32, least / len(cuts), high / len(cuts)))
        level = level * jnp.repeat(heights, shape[axis_at] // parts).reshape([-1 if axis == axis_at else 1 for axis in range(len(shape))])
    return level


def normal_values(own_key, shape, width, reach, split=(), held_as=jnp.bfloat16):
    values = width * jax.random.normal(own_key, shape, jnp.float32)
    if split:
        values = values * level_of(own_key, shape, split, -0.22, 0.18)
    return jnp.clip(values, -reach, reach).astype(held_as)


def gaussian_with(key, shape, deviation, limit, shards, heavy, kind=jnp.bfloat16):
    drawn = deviation * jax.random.normal(key, shape, jnp.float32)
    if shards:
        drawn = drawn * level_of(key, shape, shards, -0.22, 0.18)
    return jnp.clip(with_spikes(drawn, jax.random.fold_in(key, 3), *heavy), -limit, limit).astype(kind)


def setup_inputs(seed: int = 0) -> dict:
    keys = jax.random.split(jax.random.key(seed), 4)
    return {
        "points": normal_values(keys[0], (NPTS, FEAT), 1.0, 6.0, ((0, 256),)),
        "abar": gaussian_with(keys[1], (NPTS, N_ROW, N_COL, PTS), 1.0, 6.0, ((0, 16), (2, 16)), (2, 0, 16, 2.0)),
        "inv_scale": jnp.clip(jnp.exp(jax.random.uniform(keys[2], (FEAT,), jnp.float32, math.log(0.05), math.log(0.2))), 0.05, 0.2),
    }


def reference(points, abar, inv_scale):
    scaled = (points.astype(jnp.float32) * inv_scale[None, :]).astype(jnp.bfloat16)
    wide = scaled.astype(jnp.float32)
    squares = jnp.sum(wide * wide, axis=1)
    matrix = abar.reshape(NPTS, NPTS)
    block = 512 if NPTS % 512 == 0 else NPTS
    count = NPTS // block

    def one_block(carry, index):
        col_acc, col_total = carry
        start = (index * block).astype(jnp.int32)
        rows_scaled = lax.dynamic_slice_in_dim(scaled, start, block, 0)
        rows_sq = lax.dynamic_slice_in_dim(squares, start, block, 0)
        rows_ab = lax.dynamic_slice_in_dim(matrix, start, block, 0)
        inner = lax.dot_general(rows_scaled, scaled, (((1,), (1,)), ((), ())), preferred_element_type=jnp.float32)
        dist = rows_sq[:, None] + squares[None, :] - 2.0 * inner
        weighted = (rows_ab.astype(jnp.float32) * jnp.exp(-0.5 * dist)).astype(jnp.bfloat16)
        row_total = jnp.sum(weighted, axis=1, dtype=jnp.float32)
        first = row_total[:, None] * rows_scaled.astype(jnp.float32) - jnp.dot(weighted, scaled, preferred_element_type=jnp.float32)
        col_acc = col_acc + lax.dot_general(weighted, rows_scaled, (((0,), (0,)), ((), ())), preferred_element_type=jnp.float32)
        col_total = col_total + jnp.sum(weighted, axis=0, dtype=jnp.float32)
        return (col_acc, col_total), first

    init = (jnp.zeros((NPTS, FEAT), jnp.float32), jnp.zeros((NPTS,), jnp.float32))
    (col_acc, col_total), firsts = lax.scan(one_block, init, jnp.arange(count, dtype=jnp.int32))
    first = firsts.reshape(NPTS, FEAT)
    second = col_total[:, None] * wide - col_acc
    return -(first + second) * inv_scale[None, :]
```

```python
import functools

import jax
import jax.numpy as jnp
from jax import lax
from jax.experimental import pallas as pl
from jax.experimental.pallas import tpu as pltpu
from jax.sharding import PartitionSpec as P

f32, bf16 = jnp.float32, jnp.bfloat16
B = 128
N = 2048
MESH = pl.DeviceIdType.MESH
ZORDER = (0, 1, -1, 2, -2, 3, -3, 4)
ZSLOT = {d % 8: k for k, d in enumerate(ZORDER)}
PLANE = ((0, 0), (1, 0), (3, 0), (0, 1), (2, 0), (1, 1), (3, 1), (2, 1))
PSLOT = {d: k for k, d in enumerate(PLANE)}


def split3(h):
    hi = h.astype(bf16)
    rest = h - hi.astype(f32)
    mid = rest.astype(bf16)
    return hi.astype(f32), mid.astype(f32), (rest - mid.astype(f32)).astype(bf16).astype(f32)


def kernel(
    points, abar, inv_scale, out,
    rows_raw, cols_raw, inv, tile, flat, left, right_t, right, left_t, weights, prods, second_t,
    y_out, y_in, z_out, z_in, d_out, d_in, p_out, p_in, result,
    load_sem, tile_sem,
    rz_send, rz_recv, ry_send, ry_recv, cp_send, cp_recv, cd_send, cd_recv,
    y_send, y_recv, z_send, z_recv, d_send, d_recv, p_send, p_recv,
):
    row, col = lax.axis_index("row"), lax.axis_index("col")
    x, y_hi, core = row // 4, (row // 2) % 2, row % 2
    y_lo, z = col // 8, col % 8

    def at_z(d):
        return (row, y_lo * 8 + (z + d + 8) % 8)

    def plane_row(d, which):
        return ((x + d[0]) % 4) * 4 + ((y_hi + d[1]) % 2) * 2 + which

    def at_plane(d):
        return (plane_row(d, core), col)

    at_y = (row, (1 - y_lo) * 8 + z)
    at_core = (row + 1 - 2 * core, col)

    peers = [at_core, at_y] + [at_z(d) for d in ZORDER[1:]] + [at_plane(d) for d in PLANE[1:]]
    barrier = pltpu.get_barrier_semaphore()
    for peer in reversed(peers):
        pl.semaphore_signal(barrier, inc=1, device_id=peer, device_id_type=MESH)

    loads = [
        pltpu.make_async_copy(points, rows_raw.at[0], load_sem.at[0]),
        pltpu.make_async_copy(points, cols_raw.at[row], load_sem.at[1]),
        pltpu.make_async_copy(inv_scale, inv, load_sem.at[2]),
    ]
    for load in loads:
        load.start()

    def tile_rows(k):
        zk = (z + ZORDER[k] + 8) % 8
        return [(h * 8 + zk) * B for h in (y_lo, 1 - y_lo)]

    tiles = []
    for k in range(8):
        for h, start in enumerate(tile_rows(k)):
            tiles.append(
                pltpu.make_async_copy(
                    abar.at[pl.ds(start, B)],
                    tile.at[pl.ds((2 * k + h) * B, B)],
                    tile_sem.at[2 * k + h],
                )
            )
    for copy in tiles:
        copy.start()
    for load in loads:
        load.wait()

    def relayout(s):
        tiles[s].wait()

        def group(g, carry):
            at = pl.ds(pl.multiple_of(s * B + g * 16, 16), 16)
            turned = pltpu.einshape("iap->aip", tile[at])
            for a in range(16):
                flat[at, a * B : (a + 1) * B] = turned[a]
            return carry

        lax.fori_loop(0, B // 16, group, 0, unroll=2)

    for s in range(6):
        relayout(s)

    pl.semaphore_wait(barrier, len(peers))

    def remote(src, dst, send, recv, peer):
        return pltpu.make_async_remote_copy(
            src_ref=src, dst_ref=dst, send_sem=send, recv_sem=recv, device_id=peer, device_id_type=MESH
        )

    to_plane = {
        k: remote(cols_raw.at[row], cols_raw.at[row], cp_send.at[k], cp_recv.at[PSLOT[(-d[0]) % 4, d[1]]], at_plane(d))
        for k, d in enumerate(PLANE)
        if k
    }
    from_plane = {
        k: remote(cols_raw.at[row], cols_raw.at[plane_row(d, core)], cp_send.at[k], cp_recv.at[k], at_plane(d))
        for k, d in enumerate(PLANE)
        if k
    }
    to_core = {
        k: remote(
            cols_raw.at[plane_row(d, core)], cols_raw.at[plane_row(d, core)], cd_send.at[k], cd_recv.at[k], at_core
        )
        for k, d in enumerate(PLANE)
    }
    from_core = {
        k: remote(
            cols_raw.at[plane_row(d, core)], cols_raw.at[plane_row(d, 1 - core)], cd_send.at[k], cd_recv.at[k], at_core
        )
        for k, d in enumerate(PLANE)
    }
    to_z = {
        k: remote(rows_raw.at[0], rows_raw.at[2 * ZSLOT[(-d) % 8]], rz_send.at[k], rz_recv.at[ZSLOT[(-d) % 8]], at_z(d))
        for k, d in enumerate(ZORDER)
        if k
    }
    from_z = {
        k: remote(rows_raw.at[0], rows_raw.at[2 * k], rz_send.at[k], rz_recv.at[k], at_z(ZORDER[k]))
        for k in range(1, 8)
    }
    to_y = {
        k: remote(rows_raw.at[2 * k], rows_raw.at[2 * k + 1], ry_send.at[k], ry_recv.at[k], at_y) for k in range(8)
    }
    to_core[0].start()
    for k in range(1, 8):
        to_plane[k].start()
    to_y[0].start()
    for k in range(1, 8):
        to_z[k].start()

    scale = inv[...]
    lane = lax.broadcasted_iota(jnp.int32, (B, B), 1)
    sub = lax.broadcasted_iota(jnp.int32, (B, B), 0)

    def prepare_row(s):
        at = pl.ds(pl.multiple_of(s * B, B), B)
        scaled = (rows_raw[s].astype(f32) * scale).astype(bf16)
        wide = scaled.astype(f32)
        hi, mid, low = split3(jnp.broadcast_to(-0.5 * jnp.sum(wide * wide, axis=1, keepdims=True), (B, B)))
        extra = jnp.where(
            lane == 0, hi, jnp.where(lane == 1, mid, jnp.where(lane == 2, low, jnp.where(lane < 6, 1.0, 0.0)))
        )
        left[at, :B] = scaled
        left[at, B:] = extra.astype(bf16)
        left_t[:B, at] = wide.T.astype(bf16)
        left_t[B:, at] = jnp.ones((16, B), bf16)

    def prepare_col(a):
        at = pl.ds(pl.multiple_of(a * B, B), B)
        scaled = (cols_raw[a].astype(f32) * scale).astype(bf16)
        right[at, :B] = scaled
        right[at, B:] = jnp.ones((B, B), bf16)
        wide = scaled.astype(f32).T
        hi, mid, low = split3(jnp.broadcast_to(-0.5 * jnp.sum(wide * wide, axis=0, keepdims=True), (B, B)))
        extra = jnp.where(
            sub < 3,
            1.0,
            jnp.where(sub == 3, hi, jnp.where(sub == 4, mid, jnp.where(sub == 5, low, 0.0))),
        )
        right_t[:B, at] = wide.astype(bf16)
        right_t[B:, at] = extra.astype(bf16)

    prepare_col(row)
    prepare_row(0)
    for s in range(6, 16):
        relayout(s)

    for k in (1, 2):
        from_plane[k].wait_recv()
        to_core[k].start()
        from_z[k].wait_recv()
        to_y[k].start()
    for k in range(3, 8):
        from_plane[k].wait_recv()
        to_core[k].start()
    for k in range(1, 8):
        prepare_col(plane_row(PLANE[k], core))
    for k in range(8):
        from_core[k].wait_recv()
        prepare_col(plane_row(PLANE[k], 1 - core))
    to_y[0].wait_recv()
    prepare_row(1)

    second_t[...] = jnp.zeros_like(second_t)

    y_sends = {k: remote(y_out.at[k], y_in.at[k], y_send.at[k], y_recv.at[k], at_y) for k in range(8)}
    z_sends = {
        k: remote(z_out.at[k], z_in.at[ZSLOT[(-d) % 8]], z_send.at[k], z_recv.at[ZSLOT[(-d) % 8]], at_z(d))
        for k, d in enumerate(ZORDER)
        if k
    }
    z_arrive = {
        k: remote(z_out.at[k], z_in.at[k], z_send.at[k], z_recv.at[k], at_z(ZORDER[k])) for k in range(1, 8)
    }

    def first_terms(s):
        at = pl.ds(s * B, B)
        both = prods[at, :]
        return both[:, B:] * left[at, :B].astype(f32) - both[:, :B]

    def give_y(k):
        y_out[k] = first_terms(2 * k + 1).astype(bf16)

    def give_z(k):
        y_sends[k].wait_recv()
        z_out[k] = (first_terms(2 * k) + y_in[k].astype(f32)).astype(bf16)

    step_cols = 256
    for t in range(9):
        slot = t % 2
        if 3 <= t + 2 < 8:
            from_z[t + 2].wait_recv()
            to_y[t + 2].start()
        if 0 < t < 8:
            to_y[t].wait_recv()
            prepare_row(2 * t)
            prepare_row(2 * t + 1)
        at = pl.ds(t * 2 * B, 2 * B)
        before = pl.ds((t - 1) * 2 * B, 2 * B)
        total = None
        for c in range(N // step_cols):
            cs = slice(c * step_cols, (c + 1) * step_cols)
            if t < 8:
                power = jnp.dot(left[at, :], right_t[:, cs], preferred_element_type=f32)
                weights[slot, :, cs] = (flat[at, cs].astype(f32) * jnp.exp(power)).astype(bf16)
            if t > 0:
                held = weights[1 - slot, :, cs]
                part = jnp.dot(held, right[cs, :], preferred_element_type=f32)
                total = part if total is None else total + part
                second_t[:, cs] += jnp.dot(left_t[:, before], held, preferred_element_type=f32)
        if t > 0:
            prods[before, :] = total
        if t >= 2:
            y_sends[t - 2].start()
        if t >= 1:
            give_y(t - 1)
        if t >= 6 and t - 5 >= 1:
            z_sends[t - 5].start()
        if t >= 5 and t - 4 >= 1:
            give_z(t - 4)

    d_sends = {k: remote(d_out.at[k], d_in.at[k], d_send.at[k], d_recv.at[k], at_core) for k in range(8)}
    p_sends = {
        k: remote(p_out.at[k], p_in.at[PSLOT[(-d[0]) % 4, d[1]]], p_send.at[k], p_recv.at[PSLOT[(-d[0]) % 4, d[1]]], at_plane(d))
        for k, d in enumerate(PLANE)
        if k
    }
    p_arrive = {
        k: remote(p_out.at[k], p_in.at[k], p_send.at[k], p_recv.at[k], at_plane(PLANE[k])) for k in range(1, 8)
    }

    def second_terms(a):
        at = pl.ds(pl.multiple_of(a * B, B), B)
        return second_t[B : B + 1, at] * right_t[:B, at].astype(f32) - second_t[:B, at]

    for k in reversed(range(8)):
        d_out[k] = second_terms(plane_row(PLANE[k], 1 - core)).astype(bf16)
        if k < 7:
            d_sends[k + 1].start()
    d_sends[0].start()
    y_sends[7].start()
    z_sends[4].start()
    for k in reversed(range(1, 8)):
        d_sends[k].wait_recv()
        p_out[k] = (second_terms(plane_row(PLANE[k], core)) + d_in[k].astype(f32)).astype(bf16)
        if k < 7:
            p_sends[k + 1].start()
    d_sends[0].wait_recv()
    mine_t = second_terms(row) + d_in[0].astype(f32)
    p_sends[1].start()
    for k in (5, 6, 7):
        give_z(k)
        if k > 5:
            z_sends[k - 1].start()
    y_sends[0].wait_recv()
    mine = first_terms(0) + y_in[0].astype(f32)
    z_sends[7].start()
    for k in range(1, 8):
        p_arrive[k].wait_recv()
        mine_t += p_in[k].astype(f32)
    mine += mine_t.T
    for k in range(1, 8):
        z_arrive[k].wait_recv()
        mine += z_in[k].astype(f32)
    result[...] = -mine * scale
    store = pltpu.make_async_copy(result, out, load_sem.at[0])
    store.start()

    for group in (to_plane, to_core, to_z, to_y, y_sends, z_sends, d_sends, p_sends):
        for copy in group.values():
            copy.wait_send()
    store.wait()


def per_device(points, abar, inv_scale):
    vmem, dma = pltpu.VMEM, pltpu.SemaphoreType.DMA
    blocks = lambda n: vmem((n, B, B), bf16)
    return pl.pallas_call(
        kernel,
        out_shape=jax.ShapeDtypeStruct((B, B), f32),
        in_specs=[pl.BlockSpec(memory_space=pl.ANY)] * 3,
        out_specs=pl.BlockSpec(memory_space=pl.ANY),
        scratch_shapes=[
            blocks(16), blocks(16), vmem((1, B), f32),
            vmem((N, 16, B), bf16), vmem((N, N), bf16),
            vmem((N, 2 * B), bf16), vmem((2 * B, N), bf16), vmem((N, 2 * B), bf16), vmem((B + 16, N), bf16),
            vmem((2, 2 * B, N), bf16), vmem((N, 2 * B), f32), vmem((B + 16, N), f32),
            blocks(8), blocks(8), blocks(8), blocks(8), blocks(8), blocks(8), blocks(8), blocks(8),
            vmem((B, B), f32),
            dma((3,)), dma((16,)),
            *[dma((8,)) for _ in range(16)],
        ],
        compiler_params=pltpu.CompilerParams(
            collective_id=0, has_side_effects=True, vmem_limit_bytes=60 * 2**20
        ),
    )(points, abar.reshape(N, 16, B), inv_scale.reshape(1, B))


def solution(mesh):
    placed = (P(("row", "col"), None), P("row", None, "col", None), P())
    return jax.shard_map(
        per_device, mesh=mesh, in_specs=placed, out_specs=P(("row", "col"), None), check_vma=False
    )
```

```python
import functools

import jax
import jax.numpy as jnp
from jax import lax
from jax.experimental import pallas as pl
from jax.experimental.pallas import tpu as pltpu
from jax.sharding import PartitionSpec as P

f32, bf16 = jnp.float32, jnp.bfloat16
B = 128
N = 2048
MESH = pl.DeviceIdType.MESH
ZS = (0, 1, -1, 2, -2, 3, -3, 4)
PLANE = ((0, 0), (1, 0), (3, 0), (2, 0), (0, 1), (3, 1), (1, 1), (2, 1))
ACROSS = 4
ZSLOT = {d % 8: k for k, d in enumerate(ZS)}
PSLOT = {d: k for k, d in enumerate(PLANE)}
PAIRS = (
    ((2, 0), (-2, 0)),
    ((1, 1), (-1, 1)),
    ((2, 1), (-2, 1)),
    ((3, 0), (-3, 0)),
    ((3, 1), (-3, 1)),
    ((4, 0), (4, 1)),
)
LAST = ((1, 0), (-1, 0), (0, 0), (0, 1))
NEAR = 5
UNITS = (
    (0, 2, 0, NEAR),
    (2, 2, 0, NEAR),
    (4, 2, 0, NEAR),
    (6, 2, 0, NEAR),
    (0, 4, NEAR, 8),
    (4, 4, NEAR, 8),
    (8, 2, 0, 8),
    (10, 2, 0, 8),
    (12, 4, 6, 8),
    (12, 4, 4, 6),
    (12, 4, 2, 4),
    (12, 4, 0, 2),
)
GROUPS = tuple(g for pair in PAIRS for g in pair) + LAST
POS = {(d % 8, h): i for i, (d, h) in enumerate(GROUPS)}
EARLY = 12
NEXT_P = 2


def split3(h):
    hi = h.astype(bf16)
    rest = h - hi.astype(f32)
    mid = rest.astype(bf16)
    return hi.astype(f32), mid.astype(f32), (rest - mid.astype(f32)).astype(bf16).astype(f32)


def kernel(
    points, abar, inv_scale, out,
    rows_raw, cols_raw, inv, tile, flat, left, right_t, right, left_t, weights, prods, second_t,
    f_out, f_in, d_out, d_in, p_out, p_in,
    load_sem, tile_sem, sent,
    rz_recv, ry_recv, cp_recv, cd_recv, d_recv, p_recv, f_recv,
):
    row, col = lax.axis_index("row"), lax.axis_index("col")
    x, y_hi, core = row // 4, (row // 2) % 2, row % 2
    y_lo, z = col // 8, col % 8

    def at_z(d):
        return (row, y_lo * 8 + (z + d + 8) % 8)

    def plane_row(k, which):
        d = PLANE[k]
        return ((x + d[0]) % 4) * 4 + ((y_hi + d[1]) % 2) * 2 + which

    def at_plane(k):
        return (plane_row(k, core), col)

    at_y = (row, (1 - y_lo) * 8 + z)
    at_core = (row + 1 - 2 * core, col)

    peers = [at_core, at_y] + [at_z(d) for d in (1, -1, 2, -2)] + [at_plane(k) for k in (1, 2, 3, 4)]
    barrier = pltpu.get_barrier_semaphore()
    for peer in reversed(peers):
        pl.semaphore_signal(barrier, inc=1, device_id=peer, device_id_type=MESH)

    own = POS[0, 0]
    loads = [
        pltpu.make_async_copy(points, rows_raw.at[own], load_sem.at[0]),
        pltpu.make_async_copy(points, cols_raw.at[0], load_sem.at[1]),
        pltpu.make_async_copy(inv_scale, inv, load_sem.at[2]),
    ]
    for load in loads:
        load.start()
    with jax.named_scope("loads"):
        for load in loads:
            load.wait()

    tiles = []
    for s, (d, h) in enumerate(GROUPS):
        start = ((y_lo if h == 0 else 1 - y_lo) * 8 + (z + d + 8) % 8) * B
        tiles.append(pltpu.make_async_copy(abar.at[pl.ds(start, B)], tile.at[pl.ds(s * B, B)], tile_sem.at[s]))
    for copy in tiles:
        copy.start()

    with jax.named_scope("barrier"):
        pl.semaphore_wait(barrier, len(peers))

    n_sent = []

    def remote(src, dst, recv, peer):
        return pltpu.make_async_remote_copy(
            src_ref=src, dst_ref=dst, send_sem=sent, recv_sem=recv, device_id=peer, device_id_type=MESH
        )

    def start(copy):
        n_sent.append(1)
        copy.start()

    def opposite(k):
        d = PLANE[k]
        return PSLOT[(-d[0]) % 4, d[1]]

    to_plane = {
        k: remote(
            cols_raw.at[0 if k <= ACROSS else 2 * ACROSS],
            cols_raw.at[2 * opposite(k)],
            cp_recv.at[opposite(k)],
            at_plane(k if k <= ACROSS else PSLOT[PLANE[k][0], 0]),
        )
        for k in range(1, 8)
    }
    from_plane = {
        k: remote(cols_raw.at[0], cols_raw.at[2 * k], cp_recv.at[k], at_plane(1)) for k in range(1, 8)
    }
    to_core = {
        k: remote(cols_raw.at[2 * k], cols_raw.at[2 * k + 1], cd_recv.at[k], at_core) for k in range(8)
    }
    to_z = {
        d: remote(rows_raw.at[own], rows_raw.at[POS[-d % 8, 0]], rz_recv.at[ZSLOT[-d % 8]], at_z(d))
        for d in (1, -1, 2, -2)
    }
    for d in (3, -3):
        step = d // 3
        to_z[d] = remote(
            rows_raw.at[POS[-2 * step % 8, 0]], rows_raw.at[POS[-d % 8, 0]], rz_recv.at[ZSLOT[-d % 8]], at_z(step)
        )
    to_z[4] = remote(
        rows_raw.at[jnp.where(core == 0, POS[-2 % 8, 0], POS[2, 0])],
        rows_raw.at[POS[4, 0]],
        rz_recv.at[ZSLOT[4]],
        at_z(2 - 4 * core),
    )
    from_z = {
        d: remote(rows_raw.at[own], rows_raw.at[POS[d % 8, 0]], rz_recv.at[ZSLOT[d % 8]], at_z(1)) for d in ZS[1:]
    }
    to_y = {
        d: remote(rows_raw.at[POS[d % 8, 0]], rows_raw.at[POS[d % 8, 1]], ry_recv.at[ZSLOT[d % 8]], at_y) for d in ZS
    }
    start(to_core[0])
    for k in (4, 3, 1, 2):
        start(to_plane[k])
    start(to_y[0])
    for d in (1, -1, 2, -2):
        start(to_z[d])

    scale = inv[...]
    lane = lax.broadcasted_iota(jnp.int32, (B, B), 1)
    sub = lax.broadcasted_iota(jnp.int32, (16, B), 0)

    def prepare_row(s):
        at = pl.ds(s * B, B)
        scaled = (rows_raw[s].astype(f32) * scale).astype(bf16)
        wide = scaled.astype(f32)
        hi, mid, low = split3(jnp.broadcast_to(-0.5 * jnp.sum(wide * wide, axis=1, keepdims=True), (B, B)))
        extra = jnp.where(
            lane == 0, hi, jnp.where(lane == 1, mid, jnp.where(lane == 2, low, jnp.where(lane < 6, 1.0, 0.0)))
        )
        left[at, :B] = scaled
        left[at, B:] = extra.astype(bf16)
        left_t[:B, at] = wide.T.astype(bf16)
        left_t[B:, at] = jnp.ones((16, B), bf16)

    def prepare_col(a):
        at = pl.ds(a * B, B)
        scaled = (cols_raw[a].astype(f32) * scale).astype(bf16)
        right[at, :B] = scaled
        right[at, B:] = jnp.ones((B, B), bf16)
        wide = scaled.astype(f32).T
        hi, mid, low = split3(jnp.broadcast_to(-0.5 * jnp.sum(wide * wide, axis=0, keepdims=True), (16, B)))
        extra = jnp.where(
            sub < 3,
            1.0,
            jnp.where(sub == 3, hi, jnp.where(sub == 4, mid, jnp.where(sub == 5, low, 0.0))),
        )
        right_t[:B, at] = wide.astype(bf16)
        right_t[B : B + 16, at] = extra.astype(bf16)
        right_t[B + 16 :, at] = jnp.zeros((B - 16, B), bf16)

    places = []
    for a in range(16):
        dx, dy = (a // 4 - x + 4) % 4, (a // 2 % 2 - y_hi + 2) % 2
        k = jnp.int32(0)
        for i, d in enumerate(PLANE):
            k = jnp.where((dx == d[0]) & (dy == d[1]), i, k)
        places.append(pl.multiple_of((2 * k + (a % 2 - core + 2) % 2) * B, B))

    def relayout(s):
        tiles[s].wait()

        def group(g, carry):
            at = pl.ds(pl.multiple_of(s * B + g * 16, 16), 16)
            turned = pltpu.einshape("iap->aip", tile[at])
            for a in range(16):
                flat[at, pl.ds(places[a], B)] = turned[a]
            return carry

        lax.fori_loop(0, B // 16, group, 0, unroll=2)

    def arrive_z(d):
        with jax.named_scope(f"z_{d}"):
            from_z[d].wait_recv()
        start(to_y[d])

    def arrive_plane(k):
        with jax.named_scope(f"plane_{k}"):
            from_plane[k].wait_recv()
        start(to_core[k])

    with jax.named_scope("relayout"):
        prepare_col(0)
        prepare_row(own)
        for s in range(EARLY):
            relayout(s)
    arrive_plane(ACROSS)
    for k in (7, 6, 5):
        start(to_plane[k])
    for d in (1, -1):
        arrive_z(d)
    with jax.named_scope("relayout2"):
        for s in range(EARLY, 16):
            relayout(s)
    for d in (2, -2):
        arrive_z(d)
    for d in (3, -3, 4):
        start(to_z[d])
    for k in (1, 2, 3):
        arrive_plane(k)
    for k in range(1, NEAR):
        prepare_col(2 * k)
    def from_core(chips):
        with jax.named_scope(f"core_{chips[0]}"):
            for k in chips:
                to_core[k].wait_recv()
        for k in chips:
            prepare_col(2 * k + 1)

    from_core(range(NEAR))

    def f_place(g):
        d, h = g
        if h and d in (3, -3, 4):
            return (row, (1 - y_lo) * 8 + (z + d + 8) % 8)
        return at_z(d) if d else at_y

    f_sends = {
        g: remote(f_out.at[POS[g[0] % 8, g[1]]], f_in.at[POS[-g[0] % 8, g[1]]], f_recv.at[POS[-g[0] % 8, g[1]]], f_place(g))
        for g in GROUPS
        if g != (0, 0)
    }
    f_arrive = {
        g: remote(f_out.at[POS[g[0] % 8, g[1]]], f_in.at[POS[g[0] % 8, g[1]]], f_recv.at[POS[g[0] % 8, g[1]]], at_y)
        for g in GROUPS
        if g != (0, 0)
    }
    d_sends = {k: remote(d_out.at[k], d_in.at[k], d_recv.at[k], at_core) for k in range(8)}
    p_sends = {
        k: remote(
            p_out.at[k],
            p_in.at[opposite(k)],
            p_recv.at[opposite(k)],
            at_plane(k),
        )
        for k in range(1, 8)
    }
    p_arrive = {k: remote(p_out.at[k], p_in.at[k], p_recv.at[k], at_plane(1)) for k in range(1, 8)}

    def first_terms(s):
        both = prods[pl.ds(s * B, B), :]
        return both[:, B:] * left[pl.ds(s * B, B), :B].astype(f32) - both[:, :B]

    def arrived(g):
        with jax.named_scope(f"f_{g[0]}_{g[1]}"):
            f_arrive[g].wait_recv()
        return f_in[POS[g[0] % 8, g[1]]].astype(f32)

    def give_first(g):
        s = POS[g[0] % 8, g[1]]
        terms = first_terms(s)
        if g == (0, 1):
            for d in (1, -1, 2, -2):
                terms += arrived((d, 1))
        f_out[s] = terms.astype(bf16)
        pending.append(f_sends[g])

    def second_terms(a):
        at = pl.ds(a * B, B)
        return second_t[B : B + 1, at] * right_t[:B, at].astype(f32) - second_t[:B, at]

    def weigh(rows, cs):
        power = jnp.dot(left[rows, :], right_t[:, cs], preferred_element_type=f32)
        return (flat[rows, cs].astype(f32) * jnp.exp(power)).astype(bf16)

    def make_weights(u):
        first, n, low, high = UNITS[u]
        rows = pl.ds(first * B, n * B)
        for c in range(low, high):
            cs = slice(c * 2 * B, (c + 1) * 2 * B)
            weights[u % 2, : n * B, cs] = weigh(rows, cs)

    seen_rows, seen_cols = set(), set()

    def use_weights(u):
        first, n, low, high = UNITS[u]
        rows, cs = pl.ds(first * B, n * B), slice(low * 2 * B, high * 2 * B)
        held = weights[u % 2, : n * B, cs]
        part = jnp.dot(held, right[cs, :], preferred_element_type=f32)
        for at, new in ((slice(i * B, (i + 1) * B), first + i) for i in range(n)):
            to = pl.ds(new * B, B)
            if new in seen_rows:
                prods[to, :] += part[at]
            else:
                prods[to, :] = part[at]
            seen_rows.add(new)
        term = jnp.dot(left_t[:, rows], held, preferred_element_type=f32)
        if low in seen_cols:
            second_t[:, cs] += term
        else:
            second_t[:, cs] = term
        seen_cols.update(range(low, high))

    done = {GROUPS[i]: u + 1 for u, (first, n, _, _) in enumerate(UNITS) for i in range(first, first + n)}
    def need(g):
        d, h = g
        if g == (0, 0):
            return
        if h == 1:
            with jax.named_scope(f"y_{d}"):
                to_y[d].wait_recv()

    pending = []

    def flush():
        while pending:
            start(pending.pop(0))

    def give_core(k):
        d_out[k] = second_terms(2 * k + 1).astype(bf16)
        pending.append(d_sends[k])

    def give_plane(k):
        with jax.named_scope(f"d_{k}"):
            d_sends[k].wait_recv()
        terms = second_terms(2 * k) + d_in[k].astype(f32)
        p_out[k] = terms.astype(bf16)
        pending.append(p_sends[k])

    p_queue = [7, 6, 5, 4, 3, 2, 1]
    core_done = {}
    ready = {(0, 0)}

    def fresh(u):
        return [g for g in GROUPS[UNITS[u][0] : UNITS[u][0] + UNITS[u][1]] if g not in ready]

    for g in fresh(0):
        need(g)
        prepare_row(POS[g[0] % 8, g[1]])
        ready.add(g)
    for t in range(len(UNITS) + 1):
        flush()
        if t == 2:
            arrive_plane(6)
            arrive_plane(5)
            arrive_z(3)
            arrive_z(-3)
        if t == 3:
            arrive_plane(7)
            for k in range(NEAR, 8):
                prepare_col(2 * k)
        if t == 4:
            arrive_z(4)
            from_core(range(NEAR, 8))
        nexts = fresh(t + 1) if t + 1 < len(UNITS) else ()
        for g in nexts:
            need(g)
        if t < len(UNITS):
            make_weights(t)
        for g in nexts:
            prepare_row(POS[g[0] % 8, g[1]])
            ready.add(g)
        if t > 0:
            use_weights(t - 1)
        if t > 0 and UNITS[t - 1][0] == 2 * len(PAIRS):
            for k in reversed(range(*UNITS[t - 1][2:])):
                give_core(k)
                core_done[k] = t
        for g in GROUPS:
            if done[g] == t and t < len(UNITS):
                give_first(g)
        while p_queue and core_done.get(p_queue[0], t) + NEXT_P <= t:
            give_plane(p_queue.pop(0))
    flush()
    for g in ((1, 0), (-1, 0)):
        give_first(g)
        if len(pending) > 1:
            start(pending.pop(0))
    while p_queue and p_queue[0] > 1:
        give_plane(p_queue.pop(0))
        start(pending.pop(0))
    give_first((0, 1))
    start(pending.pop(0))
    give_plane(1)
    flush()
    with jax.named_scope("d_0"):
        d_sends[0].wait_recv()
    mine_t = second_terms(0) + d_in[0].astype(f32)
    mine = first_terms(own)
    flush()
    for k in reversed(range(1, 8)):
        with jax.named_scope(f"p_{k}"):
            p_arrive[k].wait_recv()
        mine_t += p_in[k].astype(f32)
    mine += mine_t.T
    for g in ((2, 0), (-2, 0), (3, 0), (-3, 0), (4, 0), (3, 1), (-3, 1), (4, 1), (1, 0), (-1, 0), (0, 1)):
        mine += arrived(g)
    out[...] = mine
    all_sent = flat.at[pl.ds(0, len(n_sent) * B * B // N)]
    with jax.named_scope("sent"):
        pltpu.make_async_copy(all_sent, all_sent, sent).wait()


def per_device(points, abar, inv_scale):
    vmem, dma = pltpu.VMEM, pltpu.SemaphoreType.DMA
    blocks = lambda n: vmem((n, B, B), bf16)
    total = pl.pallas_call(
        kernel,
        out_shape=jax.ShapeDtypeStruct((B, B), f32),
        in_specs=[pl.BlockSpec(memory_space=pltpu.HBM)] * 3,
        out_specs=pl.BlockSpec(memory_space=vmem),
        scratch_shapes=[
            blocks(16), blocks(16), vmem((1, B), f32),
            vmem((N, 16, B), bf16), vmem((N, N), bf16),
            vmem((N, 2 * B), bf16), vmem((2 * B, N), bf16), vmem((N, 2 * B), bf16), vmem((B + 16, N), bf16),
            vmem((2, 4 * B, N), bf16), vmem((N, 2 * B), f32), vmem((B + 16, N), f32),
            blocks(16), blocks(16), *[blocks(8) for _ in range(4)],
            dma((3,)), dma((16,)), dma,
            *[dma((8,)) for _ in range(6)], dma((16,)),
        ],
        compiler_params=pltpu.CompilerParams(
            collective_id=0, has_side_effects=True, vmem_limit_bytes=40 * 2**20
        ),
    )(*[pltpu.with_memory_space_constraint(v, pltpu.HBM) for v in (points, abar.reshape(N, 16, B), inv_scale.reshape(1, B))])
    return -total * inv_scale[None, :]


def solution(mesh):
    placed = (P(("row", "col"), None), P("row", None, "col", None), P())
    return jax.shard_map(
        per_device, mesh=mesh, in_specs=placed, out_specs=P(("row", "col"), None), check_vma=False
    )
```

```python
import functools

import jax
import jax.numpy as jnp
from jax import lax
from jax.experimental import pallas as pl
from jax.experimental.pallas import tpu as pltpu
from jax.sharding import PartitionSpec as P

f32, bf16 = jnp.float32, jnp.bfloat16
B = 128
N = 2048
MESH = pl.DeviceIdType.MESH
ZS = (0, 1, -1, 2, -2, 3, -3, 4)
PLANE = ((0, 0), (1, 0), (3, 0), (2, 0), (0, 1), (3, 1), (1, 1), (2, 1))
ACROSS = 4
ZSLOT = {d % 8: k for k, d in enumerate(ZS)}
PSLOT = {d: k for k, d in enumerate(PLANE)}
PAIRS = (
    ((2, 0), (-2, 0)),
    ((0, 1), (1, 0)),
    ((1, 1), (-1, 1)),
    ((2, 1), (-2, 1)),
    ((4, 0), (4, 1)),
    ((3, 1), (-3, 1)),
)
LAST = ((-1, 0), (0, 0), (3, 0), (-3, 0))
FAR = (4, 3, -3)
NEAR = 5
UNITS = (
    (0, 2, 0, NEAR),
    (2, 2, 0, NEAR),
    (4, 2, 0, NEAR),
    (6, 2, 0, NEAR),
    (0, 4, NEAR, 8),
    (4, 4, NEAR, 8),
    (8, 2, 0, 8),
    (10, 2, 0, 8),
    (12, 4, 6, 8),
    (12, 4, 4, 6),
    (12, 4, 2, 4),
    (12, 4, 0, 2),
)
GROUPS = tuple(g for pair in PAIRS for g in pair) + LAST
POS = {(d % 8, h): i for i, (d, h) in enumerate(GROUPS)}
SETS = (
    [("load", 0), ("load", 1)],
    [("inv", 0)],
    *[[("tile", s) for s in range(i, i + 4)] for i in range(0, 16, 4)],
    [("plane", 1), ("plane", 2), ("plane", 3)],
    [("plane", 4)],
    [("plane", 6), ("plane", 5)],
    [("plane", 7)],
    [("core", k) for k in range(NEAR)],
    [("core", k) for k in range(NEAR, 8)],
    [("z", 1), ("z", -1)],
    [("z", 2), ("z", -2)],
    [("z", 4), ("z", 3), ("z", -3)],
    [("y", 0)],
    [("y", 1), ("y", -1)],
    [("y", 2), ("y", -2)],
    [("y", 4)],
    [("y", 3), ("y", -3)],
    *[[("d", k + 1), ("d", k)] for k in (6, 4, 2, 0)],
    [("p", k) for k in range(1, 8)],
    [("f", (d, 1)) for d in (1, -1, 2, -2)],
    [("f", (4, 1))],
    [("f", (3, 1)), ("f", (-3, 1))],
    [("f", (d, 0)) for d in ZS[1:]] + [("f", (0, 1))],
)
COPIES = tuple(tuple(c) for c in SETS)
LATE = (2, 6, 7)
EARLY = 12
NEXT_P = 2


def split3(h):
    hi = h.astype(bf16)
    rest = h - hi.astype(f32)
    mid = rest.astype(bf16)
    return hi.astype(f32), mid.astype(f32), (rest - mid.astype(f32)).astype(bf16).astype(f32)


def kernel(
    points, abar, inv_scale, out,
    rows_raw, cols_raw, inv, tile, flat, left, right_t, right, left_t, weights, prods, second_t,
    f_out, f_in, d_out, d_in, p_out, p_in,
    sems, sent,
):
    row, col = lax.axis_index("row"), lax.axis_index("col")
    x, y_hi, core = row // 4, (row // 2) % 2, row % 2
    y_lo, z = col // 8, col % 8

    def at_z(d):
        return (row, y_lo * 8 + (z + d + 8) % 8)

    def plane_row(k, which):
        d = PLANE[k]
        return ((x + d[0]) % 4) * 4 + ((y_hi + d[1]) % 2) * 2 + which

    def at_plane(k):
        return (plane_row(k, core), col)

    at_y = (row, (1 - y_lo) * 8 + z)
    at_core = (row + 1 - 2 * core, col)

    peers = [at_core, at_y] + [at_z(d) for d in (1, -1, 2, -2)] + [at_plane(k) for k in (1, 2, 3, 4)]
    barrier = pltpu.get_barrier_semaphore()
    for peer in reversed(peers):
        pl.semaphore_signal(barrier, inc=1, device_id=peer, device_id_type=MESH)

    def sem(kind, which):
        return sems.at[next(i for i, c in enumerate(COPIES) if (kind, which) in c)]

    waited = set()

    def wait_for(kind, which):
        i = next(i for i, c in enumerate(COPIES) if (kind, which) in c)
        if i not in waited:
            waited.add(i)
            n = len(COPIES[i])
            if kind == "inv":
                held = inv
            elif kind == "tile":
                held = tile.at[pl.ds(0, n * B)]
            else:
                held = rows_raw.at[pl.ds(0, n)]
            with jax.named_scope(f"{kind}_{str(which).replace(', ', '_')}"):
                pltpu.make_async_copy(held, held, sems.at[i]).wait()

    own = POS[0, 0]
    loads = [
        pltpu.make_async_copy(points, rows_raw.at[own], sem("load", 0)),
        pltpu.make_async_copy(points, cols_raw.at[0], sem("load", 1)),
        pltpu.make_async_copy(inv_scale, inv, sem("inv", 0)),
    ]
    for load in loads:
        load.start()
    wait_for("load", 0)
    wait_for("inv", 0)

    tiles = []
    for s, (d, h) in enumerate(GROUPS):
        start = ((y_lo if h == 0 else 1 - y_lo) * 8 + (z + d + 8) % 8) * B
        tiles.append(pltpu.make_async_copy(abar.at[pl.ds(start, B)], tile.at[pl.ds(s * B, B)], sem("tile", s)))
    for copy in tiles:
        copy.start()

    with jax.named_scope("barrier"):
        pl.semaphore_wait(barrier, len(peers))

    n_sent = []

    def remote(src, dst, recv, peer):
        return pltpu.make_async_remote_copy(
            src_ref=src, dst_ref=dst, send_sem=sent, recv_sem=recv, device_id=peer, device_id_type=MESH
        )

    def start(copy):
        n_sent.append(1)
        copy.start()

    def opposite(k):
        d = PLANE[k]
        return PSLOT[(-d[0]) % 4, d[1]]

    to_plane = {
        k: remote(
            cols_raw.at[0 if k <= ACROSS else 2 * ACROSS],
            cols_raw.at[2 * opposite(k)],
            sem("plane", opposite(k)),
            at_plane(k if k <= ACROSS else PSLOT[PLANE[k][0], 0]),
        )
        for k in range(1, 8)
    }
    to_core = {
        k: remote(cols_raw.at[2 * k], cols_raw.at[2 * k + 1], sem("core", k), at_core) for k in range(8)
    }
    to_z = {
        d: remote(rows_raw.at[own], rows_raw.at[POS[-d % 8, 0]], sem("z", -d), at_z(d))
        for d in (1, -1, 2, -2)
    }
    for d in (3, -3):
        step = d // 3
        to_z[d] = remote(
            rows_raw.at[POS[-2 * step % 8, 0]], rows_raw.at[POS[-d % 8, 0]], sem("z", -d), at_z(step)
        )
    to_z[4] = remote(
        rows_raw.at[jnp.where(core == 0, POS[-2 % 8, 0], POS[2, 0])],
        rows_raw.at[POS[4, 0]],
        sem("z", 4),
        at_z(2 - 4 * core),
    )
    to_y = {
        d: remote(rows_raw.at[POS[d % 8, 0]], rows_raw.at[POS[d % 8, 1]], sem("y", d), at_y) for d in ZS
    }
    start(to_core[0])
    for k in (4, 3, 1, 2):
        start(to_plane[k])
    start(to_y[0])
    for d in (1, -1, 2, -2):
        start(to_z[d])

    scale = inv[...]
    lane = lax.broadcasted_iota(jnp.int32, (B, B), 1)
    sub = lax.broadcasted_iota(jnp.int32, (16, B), 0)

    def prepare_row(s):
        at = pl.ds(s * B, B)
        scaled = (rows_raw[s].astype(f32) * scale).astype(bf16)
        wide = scaled.astype(f32)
        hi, mid, low = split3(jnp.broadcast_to(-0.5 * jnp.sum(wide * wide, axis=1, keepdims=True), (B, B)))
        extra = jnp.where(
            lane == 0, hi, jnp.where(lane == 1, mid, jnp.where(lane == 2, low, jnp.where(lane < 6, 1.0, 0.0)))
        )
        left[at, :B] = scaled
        left[at, B:] = extra.astype(bf16)
        left_t[:B, at] = wide.T.astype(bf16)
        left_t[B:, at] = jnp.ones((16, B), bf16)

    def prepare_col(a):
        at = pl.ds(a * B, B)
        scaled = (cols_raw[a].astype(f32) * scale).astype(bf16)
        right[at, :B] = scaled
        right[at, B:] = jnp.ones((B, B), bf16)
        wide = scaled.astype(f32).T
        hi, mid, low = split3(jnp.broadcast_to(-0.5 * jnp.sum(wide * wide, axis=0, keepdims=True), (16, B)))
        extra = jnp.where(
            sub < 3,
            1.0,
            jnp.where(sub == 3, hi, jnp.where(sub == 4, mid, jnp.where(sub == 5, low, 0.0))),
        )
        right_t[:B, at] = wide.astype(bf16)
        right_t[B : B + 16, at] = extra.astype(bf16)
        right_t[B + 16 :, at] = jnp.zeros((B - 16, B), bf16)

    places = []
    for a in range(16):
        dx, dy = (a // 4 - x + 4) % 4, (a // 2 % 2 - y_hi + 2) % 2
        k = jnp.int32(0)
        for i, d in enumerate(PLANE):
            k = jnp.where((dx == d[0]) & (dy == d[1]), i, k)
        places.append(pl.multiple_of((2 * k + (a % 2 - core + 2) % 2) * B, B))

    def relayout(s):
        wait_for("tile", s)

        def group(g, carry):
            at = pl.ds(pl.multiple_of(s * B + g * 16, 16), 16)
            turned = pltpu.einshape("iap->aip", tile[at])
            for a in range(16):
                flat[at, pl.ds(places[a], B)] = turned[a]
            return carry

        lax.fori_loop(0, B // 16, group, 0, unroll=2)

    def arrive_z(d):
        wait_for("z", d)
        start(to_y[d])

    def arrive_plane(k):
        wait_for("plane", k)
        start(to_core[k])

    with jax.named_scope("relayout"):
        prepare_col(0)
        prepare_row(own)
        for s in range(EARLY):
            relayout(s)
    arrive_plane(ACROSS)
    for k in (7, 6, 5):
        start(to_plane[k])
    for k in (1, 2, 3):
        arrive_plane(k)
    for d in (1, -1):
        arrive_z(d)
    with jax.named_scope("relayout2"):
        for s in range(EARLY, 16):
            relayout(s)
    for d in (2, -2):
        arrive_z(d)
    for d in (4, 3, -3):
        start(to_z[d])
    for k in range(1, NEAR):
        prepare_col(2 * k)
    def from_core(chips):
        wait_for("core", chips[0])
        for k in chips:
            prepare_col(2 * k + 1)

    from_core(range(NEAR))

    def f_place(g):
        d, h = g
        return at_y if d == 0 or h and d in FAR else at_z(d)

    def f_from(g):
        d, h = g
        return g if h and d in FAR or d in (0, 4) else (-d, h)

    def f_slot(g):
        d, h = g
        return POS[d % 8, 1] if h and d in FAR else POS[-d % 8, h]

    f_sends = {
        g: remote(f_out.at[POS[g[0] % 8, g[1]]], f_in.at[f_slot(g)], sem("f", f_from(g)), f_place(g))
        for g in GROUPS
        if g != (0, 0)
    }
    d_sends = {k: remote(d_out.at[k], d_in.at[k], sem("d", k), at_core) for k in range(8)}
    p_sends = {
        k: remote(
            p_out.at[k],
            p_in.at[opposite(k)],
            sem("p", opposite(k)),
            at_plane(k),
        )
        for k in range(1, 8)
    }
    def first_terms(s):
        both = prods[pl.ds(s * B, B), :]
        return both[:, B:] * left[pl.ds(s * B, B), :B].astype(f32) - both[:, :B]

    def arrived(g):
        wait_for("f", g)
        return f_in[POS[g[0] % 8, g[1]]].astype(f32)

    def give_first(g):
        s = POS[g[0] % 8, g[1]]
        terms = first_terms(s)
        if g == (0, 1):
            for d in (1, -1, 2, -2):
                terms += arrived((d, 1))
        if g[0] in FAR and g[1] == 0:
            terms += arrived((g[0], 1))
        f_out[s] = terms.astype(bf16)
        pending.append(f_sends[g])

    def second_terms(a):
        at = pl.ds(a * B, B)
        return second_t[B : B + 1, at] * right_t[:B, at].astype(f32) - second_t[:B, at]

    def weigh(rows, cs):
        power = jnp.dot(left[rows, :], right_t[:, cs], preferred_element_type=f32)
        return (flat[rows, cs].astype(f32) * jnp.exp(power)).astype(bf16)

    def make_weights(u):
        first, n, low, high = UNITS[u]
        rows = pl.ds(first * B, n * B)
        for c in range(low, high):
            cs = slice(c * 2 * B, (c + 1) * 2 * B)
            weights[u % 2, : n * B, cs] = weigh(rows, cs)

    seen_rows, seen_cols = set(), set()

    def use_weights(u):
        first, n, low, high = UNITS[u]
        rows, cs = pl.ds(first * B, n * B), slice(low * 2 * B, high * 2 * B)
        held = weights[u % 2, : n * B, cs]
        part = jnp.dot(held, right[cs, :], preferred_element_type=f32)
        for at, new in ((slice(i * B, (i + 1) * B), first + i) for i in range(n)):
            to = pl.ds(new * B, B)
            if new in seen_rows:
                prods[to, :] += part[at]
            else:
                prods[to, :] = part[at]
            seen_rows.add(new)
        term = jnp.dot(left_t[:, rows], held, preferred_element_type=f32)
        if low in seen_cols:
            second_t[:, cs] += term
        else:
            second_t[:, cs] = term
        seen_cols.update(range(low, high))

    done = {GROUPS[i]: u + 1 for u, (first, n, _, _) in enumerate(UNITS) for i in range(first, first + n)}
    def need(g):
        d, h = g
        if g == (0, 0):
            return
        if h == 1:
            wait_for("y", d)

    pending = []

    def flush():
        while pending:
            start(pending.pop(0))

    def give_core(k):
        d_out[k] = second_terms(2 * k + 1).astype(bf16)
        pending.append(d_sends[k])

    def give_plane(k):
        wait_for("d", k)
        terms = second_terms(2 * k) + d_in[k].astype(f32)
        p_out[k] = terms.astype(bf16)
        pending.append(p_sends[k])

    p_queue = [7, 6, 5, 4, 3, 2, 1]
    core_done = {}
    ready = {(0, 0)}

    def fresh(u):
        return [g for g in GROUPS[UNITS[u][0] : UNITS[u][0] + UNITS[u][1]] if g not in ready]

    for g in fresh(0):
        need(g)
        prepare_row(POS[g[0] % 8, g[1]])
        ready.add(g)
    for t in range(len(UNITS) + 1):
        flush()
        if t == 2:
            arrive_plane(6)
            arrive_plane(5)
        if t == 4:
            from_core(range(NEAR, 8))
        if t == 3:
            for k in range(NEAR, 8):
                prepare_col(2 * k)
        nexts = []
        for u in (t, t + 1):
            if u < len(UNITS) and (u == t or u not in LATE):
                for g in fresh(u):
                    need(g)
                    ready.add(g)
                    if u == t:
                        prepare_row(POS[g[0] % 8, g[1]])
                    else:
                        nexts.append(g)
        if t == 2:
            arrive_plane(7)
            for d in (4, 3, -3):
                arrive_z(d)
        if t < len(UNITS):
            make_weights(t)
        for g in nexts:
            prepare_row(POS[g[0] % 8, g[1]])
        if t > 0:
            use_weights(t - 1)
        if t > 0 and UNITS[t - 1][0] == 2 * len(PAIRS):
            for k in reversed(range(*UNITS[t - 1][2:])):
                give_core(k)
                core_done[k] = t
        for g in GROUPS:
            if done[g] == t and t < len(UNITS) and g not in ((0, 1), (4, 0)):
                give_first(g)
        while p_queue and core_done.get(p_queue[0], t) + NEXT_P <= t:
            give_plane(p_queue.pop(0))
    flush()
    while p_queue and p_queue[0] > 3:
        give_plane(p_queue.pop(0))
        if len(pending) > 1:
            start(pending.pop(0))
    for g in ((4, 0), (3, 0), (-3, 0)):
        give_first(g)
        if len(pending) > 1:
            start(pending.pop(0))
    while p_queue and p_queue[0] > 1:
        give_plane(p_queue.pop(0))
        start(pending.pop(0))
    for g in ((-1, 0), (0, 1)):
        give_first(g)
        start(pending.pop(0))
    give_plane(1)
    flush()
    wait_for("d", 0)
    mine_t = second_terms(0) + d_in[0].astype(f32)
    mine = first_terms(own)
    flush()
    for k in reversed(range(1, 8)):
        wait_for("p", k)
        mine_t += p_in[k].astype(f32)
    mine += mine_t.T
    for g in ((2, 0), (-2, 0), (1, 0), (-1, 0), (0, 1), (3, 0), (-3, 0), (4, 0)):
        mine += arrived(g)
    out[...] = mine
    all_sent = flat.at[pl.ds(0, len(n_sent) * B * B // N)]
    with jax.named_scope("sent"):
        pltpu.make_async_copy(all_sent, all_sent, sent).wait()


def per_device(points, abar, inv_scale):
    vmem, dma = pltpu.VMEM, pltpu.SemaphoreType.DMA
    blocks = lambda n: vmem((n, B, B), bf16)
    total = pl.pallas_call(
        kernel,
        out_shape=jax.ShapeDtypeStruct((B, B), f32),
        in_specs=[pl.BlockSpec(memory_space=pltpu.HBM)] * 3,
        out_specs=pl.BlockSpec(memory_space=vmem),
        scratch_shapes=[
            blocks(16), blocks(16), vmem((1, B), f32),
            vmem((N, 16, B), bf16), vmem((N, N), bf16),
            vmem((N, 2 * B), bf16), vmem((2 * B, N), bf16), vmem((N, 2 * B), bf16), vmem((B + 16, N), bf16),
            vmem((2, 4 * B, N), bf16), vmem((N, 2 * B), f32), vmem((B + 16, N), f32),
            blocks(16), blocks(16), *[blocks(8) for _ in range(4)],
            dma((len(COPIES),)), dma,
        ],
        compiler_params=pltpu.CompilerParams(
            collective_id=0, has_side_effects=True, vmem_limit_bytes=40 * 2**20
        ),
    )(*[pltpu.with_memory_space_constraint(v, pltpu.HBM) for v in (points, abar.reshape(N, 16, B), inv_scale.reshape(1, B))])
    return -total * inv_scale[None, :]


def solution(mesh):
    placed = (P(("row", "col"), None), P("row", None, "col", None), P())
    return jax.shard_map(
        per_device, mesh=mesh, in_specs=placed, out_specs=P(("row", "col"), None), check_vma=False
    )
```

```python
import functools

import jax
import jax.numpy as jnp
from jax import lax
from jax.experimental import pallas as pl
from jax.experimental.pallas import tpu as pltpu
from jax.sharding import PartitionSpec as P

f32, bf16 = jnp.float32, jnp.bfloat16
B = 128
N = 2048
MESH = pl.DeviceIdType.MESH
ZS = (0, 1, -1, 2, -2, 3, -3, 4)
PLANE = ((0, 0), (1, 0), (3, 0), (2, 0), (0, 1), (3, 1), (1, 1), (2, 1))
ACROSS = 4
ZSLOT = {d % 8: k for k, d in enumerate(ZS)}
PSLOT = {d: k for k, d in enumerate(PLANE)}
PAIRS = (
    ((2, 0), (-2, 0)),
    ((0, 1), (1, 0)),
    ((1, 1), (-1, 1)),
    ((2, 1), (-2, 1)),
    ((4, 0), (4, 1)),
    ((3, 1), (-3, 1)),
)
LAST = ((-1, 0), (0, 0), (3, 0), (-3, 0))
FAR = (4, 3, -3)
NEAR = 5
UNITS = (
    (0, 2, 0, NEAR),
    (2, 2, 0, NEAR),
    (4, 2, 0, NEAR),
    (6, 2, 0, NEAR),
    (0, 4, NEAR, 8),
    (4, 4, NEAR, 8),
    (8, 2, 0, 8),
    (10, 2, 0, 8),
    (12, 4, 6, 8),
    (12, 4, 4, 6),
    (12, 4, 2, 4),
    (12, 4, 0, 2),
)
GROUPS = tuple(g for pair in PAIRS for g in pair) + LAST
POS = {(d % 8, h): i for i, (d, h) in enumerate(GROUPS)}
SETS = (
    [("load", 0), ("load", 1)],
    [("inv", 0)],
    *[[("tile", s) for s in range(i, i + 4)] for i in range(0, 16, 4)],
    [("plane", 1), ("plane", 2), ("plane", 3)],
    [("plane", 4)],
    [("plane", 6), ("plane", 5)],
    [("plane", 7)],
    [("core", k) for k in range(NEAR)],
    [("core", k) for k in range(NEAR, 8)],
    [("z", 1), ("z", -1)],
    [("z", 2), ("z", -2)],
    [("z", 4), ("z", 3), ("z", -3)],
    [("y", 0)],
    [("y", 1), ("y", -1)],
    [("y", 2), ("y", -2)],
    [("y", 4)],
    [("y", 3), ("y", -3)],
    *[[("d", k + 1), ("d", k)] for k in (6, 4, 2, 0)],
    [("p", k) for k in range(1, 8)],
    [("f", (d, 1)) for d in (1, -1, 2, -2)],
    [("f", (4, 1))],
    [("f", (3, 1)), ("f", (-3, 1))],
    [("f", (d, 0)) for d in ZS[1:]] + [("f", (0, 1))],
)
COPIES = tuple(tuple(c) for c in SETS)
LATE = (2, 6, 7)
EXTRA = {3: (-1, 0), 4: (3, 0), 5: (-3, 0)}
EARLY = 12
NEXT_P = 2


def split3(h):
    hi = h.astype(bf16)
    rest = h - hi.astype(f32)
    mid = rest.astype(bf16)
    return hi.astype(f32), mid.astype(f32), (rest - mid.astype(f32)).astype(bf16).astype(f32)


def kernel(
    points, abar, inv_scale, out,
    rows_raw, cols_raw, inv, tile, flat, left, right_t, right, left_t, weights, prods, second_t,
    f_out, f_in, d_out, d_in, p_out, p_in,
    sems, sent,
):
    row, col = lax.axis_index("row"), lax.axis_index("col")
    x, y_hi, core = row // 4, (row // 2) % 2, row % 2
    y_lo, z = col // 8, col % 8

    def at_z(d):
        return (row, y_lo * 8 + (z + d + 8) % 8)

    def plane_row(k, which):
        d = PLANE[k]
        return ((x + d[0]) % 4) * 4 + ((y_hi + d[1]) % 2) * 2 + which

    def at_plane(k):
        return (plane_row(k, core), col)

    at_y = (row, (1 - y_lo) * 8 + z)
    at_core = (row + 1 - 2 * core, col)

    peers = [at_core, at_y] + [at_z(d) for d in (1, -1, 2, -2)] + [at_plane(k) for k in (1, 2, 3, 4)]
    barrier = pltpu.get_barrier_semaphore()
    for peer in reversed(peers):
        pl.semaphore_signal(barrier, inc=1, device_id=peer, device_id_type=MESH)

    def sem(kind, which):
        return sems.at[next(i for i, c in enumerate(COPIES) if (kind, which) in c)]

    waited = set()

    def wait_for(kind, which):
        i = next(i for i, c in enumerate(COPIES) if (kind, which) in c)
        if i not in waited:
            waited.add(i)
            n = len(COPIES[i])
            if kind == "inv":
                held = inv
            elif kind == "tile":
                held = tile.at[pl.ds(0, n * B)]
            else:
                held = rows_raw.at[pl.ds(0, n)]
            with jax.named_scope(f"{kind}_{str(which).replace(', ', '_')}"):
                pltpu.make_async_copy(held, held, sems.at[i]).wait()

    own = POS[0, 0]
    loads = [
        pltpu.make_async_copy(points, rows_raw.at[own], sem("load", 0)),
        pltpu.make_async_copy(points, cols_raw.at[0], sem("load", 1)),
        pltpu.make_async_copy(inv_scale, inv, sem("inv", 0)),
    ]
    for load in loads:
        load.start()
    wait_for("load", 0)
    wait_for("inv", 0)

    tiles = []
    for s, (d, h) in enumerate(GROUPS):
        start = ((y_lo if h == 0 else 1 - y_lo) * 8 + (z + d + 8) % 8) * B
        tiles.append(pltpu.make_async_copy(abar.at[pl.ds(start, B)], tile.at[pl.ds(s * B, B)], sem("tile", s)))
    for copy in tiles:
        copy.start()

    with jax.named_scope("barrier"):
        pl.semaphore_wait(barrier, len(peers))

    n_sent = []

    def remote(src, dst, recv, peer):
        return pltpu.make_async_remote_copy(
            src_ref=src, dst_ref=dst, send_sem=sent, recv_sem=recv, device_id=peer, device_id_type=MESH
        )

    def start(copy):
        n_sent.append(1)
        copy.start()

    def opposite(k):
        d = PLANE[k]
        return PSLOT[(-d[0]) % 4, d[1]]

    to_plane = {
        k: remote(
            cols_raw.at[0 if k <= ACROSS else 2 * ACROSS],
            cols_raw.at[2 * opposite(k)],
            sem("plane", opposite(k)),
            at_plane(k if k <= ACROSS else PSLOT[PLANE[k][0], 0]),
        )
        for k in range(1, 8)
    }
    to_core = {
        k: remote(cols_raw.at[2 * k], cols_raw.at[2 * k + 1], sem("core", k), at_core) for k in range(8)
    }
    to_z = {
        d: remote(rows_raw.at[own], rows_raw.at[POS[-d % 8, 0]], sem("z", -d), at_z(d))
        for d in (1, -1, 2, -2)
    }
    for d in (3, -3):
        step = d // 3
        to_z[d] = remote(
            rows_raw.at[POS[-2 * step % 8, 0]], rows_raw.at[POS[-d % 8, 0]], sem("z", -d), at_z(step)
        )
    to_z[4] = remote(
        rows_raw.at[jnp.where(core == 0, POS[-2 % 8, 0], POS[2, 0])],
        rows_raw.at[POS[4, 0]],
        sem("z", 4),
        at_z(2 - 4 * core),
    )
    to_y = {
        d: remote(rows_raw.at[POS[d % 8, 0]], rows_raw.at[POS[d % 8, 1]], sem("y", d), at_y) for d in ZS
    }
    start(to_core[0])
    for k in (4, 3, 1, 2):
        start(to_plane[k])
    start(to_y[0])
    for d in (1, -1, 2, -2):
        start(to_z[d])

    scale = inv[...]
    lane = lax.broadcasted_iota(jnp.int32, (B, B), 1)
    sub = lax.broadcasted_iota(jnp.int32, (16, B), 0)

    def prepare_row(s):
        at = pl.ds(s * B, B)
        scaled = (rows_raw[s].astype(f32) * scale).astype(bf16)
        wide = scaled.astype(f32)
        hi, mid, low = split3(jnp.broadcast_to(-0.5 * jnp.sum(wide * wide, axis=1, keepdims=True), (B, B)))
        extra = jnp.where(
            lane == 0, hi, jnp.where(lane == 1, mid, jnp.where(lane == 2, low, jnp.where(lane < 6, 1.0, 0.0)))
        )
        left[at, :B] = scaled
        left[at, B:] = extra.astype(bf16)
        left_t[:B, at] = wide.T.astype(bf16)
        left_t[B:, at] = jnp.ones((16, B), bf16)

    def prepare_col(a):
        at = pl.ds(a * B, B)
        scaled = (cols_raw[a].astype(f32) * scale).astype(bf16)
        right[at, :B] = scaled
        right[at, B:] = jnp.ones((B, B), bf16)
        wide = scaled.astype(f32).T
        hi, mid, low = split3(jnp.broadcast_to(-0.5 * jnp.sum(wide * wide, axis=0, keepdims=True), (16, B)))
        extra = jnp.where(
            sub < 3,
            1.0,
            jnp.where(sub == 3, hi, jnp.where(sub == 4, mid, jnp.where(sub == 5, low, 0.0))),
        )
        right_t[:B, at] = wide.astype(bf16)
        right_t[B : B + 16, at] = extra.astype(bf16)
        right_t[B + 16 :, at] = jnp.zeros((B - 16, B), bf16)

    places = []
    for a in range(16):
        dx, dy = (a // 4 - x + 4) % 4, (a // 2 % 2 - y_hi + 2) % 2
        k = jnp.int32(0)
        for i, d in enumerate(PLANE):
            k = jnp.where((dx == d[0]) & (dy == d[1]), i, k)
        places.append(pl.multiple_of((2 * k + (a % 2 - core + 2) % 2) * B, B))

    def relayout(s):
        wait_for("tile", s)

        def group(g, carry):
            at = pl.ds(pl.multiple_of(s * B + g * 16, 16), 16)
            turned = pltpu.einshape("iap->aip", tile[at])
            for a in range(16):
                flat[at, pl.ds(places[a], B)] = turned[a]
            return carry

        lax.fori_loop(0, B // 16, group, 0, unroll=2)

    def arrive_z(d):
        wait_for("z", d)
        start(to_y[d])

    def arrive_plane(k):
        wait_for("plane", k)
        start(to_core[k])

    with jax.named_scope("relayout"):
        prepare_col(0)
        prepare_row(own)
        for s in range(EARLY):
            relayout(s)
    arrive_plane(ACROSS)
    for k in (7, 6, 5):
        start(to_plane[k])
    for k in (1, 2, 3):
        arrive_plane(k)
    for d in (1, -1):
        arrive_z(d)
    for d in (2, -2):
        arrive_z(d)
    for d in (4, 3, -3):
        start(to_z[d])
    with jax.named_scope("relayout2"):
        for s in range(EARLY, 16):
            relayout(s)
    for k in range(1, NEAR):
        prepare_col(2 * k)
    def from_core(chips):
        wait_for("core", chips[0])
        for k in chips:
            prepare_col(2 * k + 1)

    from_core(range(NEAR))

    def f_place(g):
        d, h = g
        return at_y if d == 0 or h and d in FAR else at_z(d)

    def f_from(g):
        d, h = g
        return g if h and d in FAR or d in (0, 4) else (-d, h)

    def f_slot(g):
        d, h = g
        return POS[d % 8, 1] if h and d in FAR else POS[-d % 8, h]

    f_sends = {
        g: remote(f_out.at[POS[g[0] % 8, g[1]]], f_in.at[f_slot(g)], sem("f", f_from(g)), f_place(g))
        for g in GROUPS
        if g != (0, 0)
    }
    d_sends = {k: remote(d_out.at[k], d_in.at[k], sem("d", k), at_core) for k in range(8)}
    p_sends = {
        k: remote(
            p_out.at[k],
            p_in.at[opposite(k)],
            sem("p", opposite(k)),
            at_plane(k),
        )
        for k in range(1, 8)
    }
    def first_terms(s):
        both = prods[pl.ds(s * B, B), :]
        return both[:, B:] * left[pl.ds(s * B, B), :B].astype(f32) - both[:, :B]

    def arrived(g):
        wait_for("f", g)
        return f_in[POS[g[0] % 8, g[1]]].astype(f32)

    def give_first(g):
        s = POS[g[0] % 8, g[1]]
        terms = first_terms(s)
        if g == (0, 1):
            for d in (1, -1, 2, -2):
                terms += arrived((d, 1))
        if g[0] in FAR and g[1] == 0:
            terms += arrived((g[0], 1))
        f_out[s] = terms.astype(bf16)
        pending.append(f_sends[g])

    def second_terms(a):
        at = pl.ds(a * B, B)
        return second_t[B : B + 1, at] * right_t[:B, at].astype(f32) - second_t[:B, at]

    def weigh(rows, cs):
        power = jnp.dot(left[rows, :], right_t[:, cs], preferred_element_type=f32)
        return (flat[rows, cs].astype(f32) * jnp.exp(power)).astype(bf16)

    def make_weights(u):
        first, n, low, high = UNITS[u]
        rows = pl.ds(first * B, n * B)
        for c in range(low, high):
            cs = slice(c * 2 * B, (c + 1) * 2 * B)
            weights[u % 2, : n * B, cs] = weigh(rows, cs)

    seen_rows, seen_cols = set(), set()

    def use_weights(u):
        first, n, low, high = UNITS[u]
        rows, cs = pl.ds(first * B, n * B), slice(low * 2 * B, high * 2 * B)
        held = weights[u % 2, : n * B, cs]
        for i in range(0, n, 2):
            part = jnp.dot(held[i * B : (i + 2) * B], right[cs, :], preferred_element_type=f32)
            to = pl.ds((first + i) * B, 2 * B)
            if first + i in seen_rows:
                prods[to, :] += part
            else:
                prods[to, :] = part
            seen_rows.add(first + i)
        term = jnp.dot(left_t[:, rows], held, preferred_element_type=f32)
        if low in seen_cols:
            second_t[:, cs] += term
        else:
            second_t[:, cs] = term
        seen_cols.update(range(low, high))

    done = {GROUPS[i]: u + 1 for u, (first, n, _, _) in enumerate(UNITS) for i in range(first, first + n)}
    def need(g):
        d, h = g
        if g == (0, 0):
            return
        if h == 1:
            wait_for("y", d)

    pending = []

    def flush():
        while pending:
            start(pending.pop(0))

    def give_core(k):
        d_out[k] = second_terms(2 * k + 1).astype(bf16)
        pending.append(d_sends[k])

    def give_plane(k):
        wait_for("d", k)
        terms = second_terms(2 * k) + d_in[k].astype(f32)
        p_out[k] = terms.astype(bf16)
        pending.append(p_sends[k])

    p_queue = [7, 6, 5, 4, 3, 2, 1]
    core_done = {}
    ready = {(0, 0)}

    def fresh(u):
        return [g for g in GROUPS[UNITS[u][0] : UNITS[u][0] + UNITS[u][1]] if g not in ready]

    for g in fresh(0):
        need(g)
        prepare_row(POS[g[0] % 8, g[1]])
        ready.add(g)
    for t in range(len(UNITS) + 1):
        flush()
        if t == 2:
            arrive_plane(6)
            arrive_plane(5)
        if t == 4:
            from_core(range(NEAR, 8))
        if t == 3:
            for k in range(NEAR, 8):
                prepare_col(2 * k)
        nexts = []
        for u in (t, t + 1):
            if u < len(UNITS) and (u == t or u not in LATE):
                for g in fresh(u):
                    need(g)
                    ready.add(g)
                    if u == t:
                        prepare_row(POS[g[0] % 8, g[1]])
                    else:
                        nexts.append(g)
        if t in EXTRA:
            nexts.append(EXTRA[t])
            ready.add(EXTRA[t])
        if t == 2:
            arrive_plane(7)
            for d in (4, 3, -3):
                arrive_z(d)
        if t < len(UNITS):
            make_weights(t)
        for g in nexts:
            prepare_row(POS[g[0] % 8, g[1]])
        if t > 0:
            use_weights(t - 1)
        if t > 0 and UNITS[t - 1][0] == 2 * len(PAIRS):
            for k in reversed(range(*UNITS[t - 1][2:])):
                give_core(k)
                core_done[k] = t
        for g in GROUPS:
            if done[g] == t and t < len(UNITS) and g not in ((0, 1), (4, 0)):
                give_first(g)
        while p_queue and core_done.get(p_queue[0], t) + NEXT_P <= t:
            give_plane(p_queue.pop(0))
    flush()
    while p_queue and p_queue[0] > 3:
        give_plane(p_queue.pop(0))
        if len(pending) > 1:
            start(pending.pop(0))
    for g in ((4, 0), (3, 0), (-3, 0)):
        give_first(g)
        if len(pending) > 1:
            start(pending.pop(0))
    while p_queue and p_queue[0] > 1:
        give_plane(p_queue.pop(0))
        start(pending.pop(0))
    give_first((-1, 0))
    start(pending.pop(0))
    give_plane(1)
    flush()
    mine_t = second_terms(0) + d_in[0].astype(f32)
    mine = first_terms(own)
    flush()
    give_first((0, 1))
    flush()
    for k in reversed(range(1, 8)):
        wait_for("p", k)
        mine_t += p_in[k].astype(f32)
    mine += mine_t.T
    for g in ((2, 0), (-2, 0), (1, 0), (-1, 0), (0, 1), (3, 0), (-3, 0), (4, 0)):
        mine += arrived(g)
    out[...] = mine
    all_sent = flat.at[pl.ds(0, len(n_sent) * B * B // N)]
    with jax.named_scope("sent"):
        pltpu.make_async_copy(all_sent, all_sent, sent).wait()


def per_device(points, abar, inv_scale):
    vmem, dma = pltpu.VMEM, pltpu.SemaphoreType.DMA
    blocks = lambda n: vmem((n, B, B), bf16)
    total = pl.pallas_call(
        kernel,
        out_shape=jax.ShapeDtypeStruct((B, B), f32),
        in_specs=[pl.BlockSpec(memory_space=pltpu.HBM)] * 3,
        out_specs=pl.BlockSpec(memory_space=vmem),
        scratch_shapes=[
            blocks(16), blocks(16), vmem((1, B), f32),
            vmem((N, 16, B), bf16), vmem((N, N), bf16),
            vmem((N, 2 * B), bf16), vmem((2 * B, N), bf16), vmem((N, 2 * B), bf16), vmem((B + 16, N), bf16),
            vmem((2, 4 * B, N), bf16), vmem((N, 2 * B), f32), vmem((B + 16, N), f32),
            blocks(16), blocks(16), *[blocks(8) for _ in range(4)],
            dma((len(COPIES),)), dma,
        ],
        compiler_params=pltpu.CompilerParams(
            collective_id=0, has_side_effects=True, vmem_limit_bytes=40 * 2**20
        ),
    )(*[pltpu.with_memory_space_constraint(v, pltpu.HBM) for v in (points, abar.reshape(N, 16, B), inv_scale.reshape(1, B))])
    return -total * inv_scale[None, :]


def solution(mesh):
    placed = (P(("row", "col"), None), P("row", None, "col", None), P())
    return jax.shard_map(
        per_device, mesh=mesh, in_specs=placed, out_specs=P(("row", "col"), None), check_vma=False
    )
```

```python
import functools

import jax
import jax.numpy as jnp
from jax import lax
from jax.experimental import pallas as pl
from jax.experimental.pallas import tpu as pltpu
from jax.sharding import PartitionSpec as P

f32, bf16 = jnp.float32, jnp.bfloat16
B = 128
N = 2048
MESH = pl.DeviceIdType.MESH
ZS = (0, 1, -1, 2, -2, 3, -3, 4)
PLANE = ((0, 0), (1, 0), (3, 0), (2, 0), (0, 1), (3, 1), (1, 1), (2, 1))
ACROSS = 4
ZSLOT = {d % 8: k for k, d in enumerate(ZS)}
PSLOT = {d: k for k, d in enumerate(PLANE)}
PAIRS = (
    ((2, 0), (-2, 0)),
    ((0, 1), (1, 0)),
    ((1, 1), (-1, 1)),
    ((2, 1), (-2, 1)),
    ((4, 0), (4, 1)),
    ((3, 1), (-3, 1)),
)
LAST = ((-1, 0), (0, 0), (3, 0), (-3, 0))
FAR = (4, 3, -3)
NEAR = 5
UNITS = (
    (0, 2, 0, NEAR),
    (2, 2, 0, NEAR),
    (4, 2, 0, NEAR),
    (6, 2, 0, NEAR),
    (0, 4, NEAR, 8),
    (4, 4, NEAR, 8),
    (8, 2, 0, 8),
    (10, 2, 0, 8),
    (12, 4, 6, 8),
    (12, 4, 4, 6),
    (12, 4, 2, 4),
    (12, 4, 0, 2),
)
GROUPS = tuple(g for pair in PAIRS for g in pair) + LAST
POS = {(d % 8, h): i for i, (d, h) in enumerate(GROUPS)}
SETS = (
    [("load", 0), ("load", 1)],
    [("inv", 0)],
    *[[("tile", s) for s in range(i, i + 4)] for i in range(0, 16, 4)],
    [("plane", 1), ("plane", 2), ("plane", 3)],
    [("plane", 4)],
    [("plane", 6), ("plane", 5)],
    [("plane", 7)],
    [("core", k) for k in range(NEAR)],
    [("core", k) for k in range(NEAR, 8)],
    [("z", 1), ("z", -1)],
    [("z", 2), ("z", -2)],
    [("z", 4), ("z", 3), ("z", -3)],
    [("y", 0)],
    [("y", 1), ("y", -1)],
    [("y", 2), ("y", -2)],
    [("y", 4)],
    [("y", 3), ("y", -3)],
    *[[("d", k + 1), ("d", k)] for k in (6, 4, 2, 0)],
    [("p", k) for k in range(1, 8)],
    [("f", (d, 1)) for d in (1, -1, 2, -2)],
    [("f", (4, 1))],
    [("f", (3, 1)), ("f", (-3, 1))],
    [("f", (d, 0)) for d in ZS[1:]] + [("f", (0, 1))],
)
COPIES = tuple(tuple(c) for c in SETS)
LATE = (2, 6, 7)
EXTRA = {3: (-1, 0), 4: (3, 0), 5: (-3, 0)}
EARLY = 12
NEXT_P = 2


def split3(h):
    hi = h.astype(bf16)
    rest = h - hi.astype(f32)
    mid = rest.astype(bf16)
    return hi.astype(f32), mid.astype(f32), (rest - mid.astype(f32)).astype(bf16).astype(f32)


def kernel(
    points, abar, inv_scale, out,
    rows_raw, cols_raw, inv, tile, flat, left, right_t, right, left_t, weights, prods, second_t,
    f_out, f_in, d_out, d_in, p_out, p_in,
    sems, sent,
):
    row, col = lax.axis_index("row"), lax.axis_index("col")
    x, y_hi, core = row // 4, (row // 2) % 2, row % 2
    y_lo, z = col // 8, col % 8

    def at_z(d):
        return (row, y_lo * 8 + (z + d + 8) % 8)

    def plane_row(k, which):
        d = PLANE[k]
        return ((x + d[0]) % 4) * 4 + ((y_hi + d[1]) % 2) * 2 + which

    def at_plane(k):
        return (plane_row(k, core), col)

    at_y = (row, (1 - y_lo) * 8 + z)
    at_core = (row + 1 - 2 * core, col)

    peers = [at_core, at_y] + [at_z(d) for d in (1, -1, 2, -2)] + [at_plane(k) for k in (1, 2, 3, 4)]
    barrier = pltpu.get_barrier_semaphore()
    for peer in reversed(peers):
        pl.semaphore_signal(barrier, inc=1, device_id=peer, device_id_type=MESH)

    def sem(kind, which):
        return sems.at[next(i for i, c in enumerate(COPIES) if (kind, which) in c)]

    waited = set()

    def wait_for(kind, which):
        i = next(i for i, c in enumerate(COPIES) if (kind, which) in c)
        if i not in waited:
            waited.add(i)
            n = len(COPIES[i])
            if kind == "inv":
                held = inv
            elif kind == "tile":
                held = tile.at[pl.ds(0, n * B)]
            else:
                held = rows_raw.at[pl.ds(0, n)]
            with jax.named_scope(f"{kind}_{str(which).replace(', ', '_')}"):
                pltpu.make_async_copy(held, held, sems.at[i]).wait()

    own = POS[0, 0]
    loads = [
        pltpu.make_async_copy(points, rows_raw.at[own], sem("load", 0)),
        pltpu.make_async_copy(points, cols_raw.at[0], sem("load", 1)),
        pltpu.make_async_copy(inv_scale, inv, sem("inv", 0)),
    ]
    for load in loads:
        load.start()
    wait_for("load", 0)
    wait_for("inv", 0)

    tiles = []
    for s, (d, h) in enumerate(GROUPS):
        start = ((y_lo if h == 0 else 1 - y_lo) * 8 + (z + d + 8) % 8) * B
        tiles.append(pltpu.make_async_copy(abar.at[pl.ds(start, B)], tile.at[pl.ds(s * B, B)], sem("tile", s)))
    for copy in tiles:
        copy.start()

    with jax.named_scope("barrier"):
        pl.semaphore_wait(barrier, len(peers))

    n_sent = []

    def remote(src, dst, recv, peer):
        return pltpu.make_async_remote_copy(
            src_ref=src, dst_ref=dst, send_sem=sent, recv_sem=recv, device_id=peer, device_id_type=MESH
        )

    def start(copy):
        n_sent.append(1)
        copy.start()

    def opposite(k):
        d = PLANE[k]
        return PSLOT[(-d[0]) % 4, d[1]]

    to_plane = {
        k: remote(
            cols_raw.at[0 if k <= ACROSS else 2 * ACROSS],
            cols_raw.at[2 * opposite(k)],
            sem("plane", opposite(k)),
            at_plane(k if k <= ACROSS else PSLOT[PLANE[k][0], 0]),
        )
        for k in range(1, 8)
    }
    to_core = {
        k: remote(cols_raw.at[2 * k], cols_raw.at[2 * k + 1], sem("core", k), at_core) for k in range(8)
    }
    to_z = {
        d: remote(rows_raw.at[own], rows_raw.at[POS[-d % 8, 0]], sem("z", -d), at_z(d))
        for d in (1, -1, 2, -2)
    }
    for d in (3, -3):
        step = d // 3
        to_z[d] = remote(
            rows_raw.at[POS[-2 * step % 8, 0]], rows_raw.at[POS[-d % 8, 0]], sem("z", -d), at_z(step)
        )
    to_z[4] = remote(
        rows_raw.at[jnp.where(core == 0, POS[-2 % 8, 0], POS[2, 0])],
        rows_raw.at[POS[4, 0]],
        sem("z", 4),
        at_z(2 - 4 * core),
    )
    to_y = {
        d: remote(rows_raw.at[POS[d % 8, 0]], rows_raw.at[POS[d % 8, 1]], sem("y", d), at_y) for d in ZS
    }
    start(to_core[0])
    for k in (4, 3, 1, 2):
        start(to_plane[k])
    start(to_y[0])
    for d in (1, -1, 2, -2):
        start(to_z[d])

    scale = inv[...]
    lane = lax.broadcasted_iota(jnp.int32, (B, B), 1)
    sub = lax.broadcasted_iota(jnp.int32, (16, B), 0)

    def prepare_row(s):
        at = pl.ds(s * B, B)
        scaled = (rows_raw[s].astype(f32) * scale).astype(bf16)
        wide = scaled.astype(f32)
        hi, mid, low = split3(jnp.broadcast_to(-0.5 * jnp.sum(wide * wide, axis=1, keepdims=True), (B, B)))
        extra = jnp.where(
            lane == 0, hi, jnp.where(lane == 1, mid, jnp.where(lane == 2, low, jnp.where(lane < 6, 1.0, 0.0)))
        )
        left[at, :B] = scaled
        left[at, B:] = extra.astype(bf16)
        left_t[:B, at] = wide.T.astype(bf16)
        left_t[B:, at] = jnp.ones((16, B), bf16)

    def prepare_col(a):
        at = pl.ds(a * B, B)
        scaled = (cols_raw[a].astype(f32) * scale).astype(bf16)
        right[at, :B] = scaled
        right[at, B:] = jnp.ones((B, B), bf16)
        wide = scaled.astype(f32).T
        hi, mid, low = split3(jnp.broadcast_to(-0.5 * jnp.sum(wide * wide, axis=0, keepdims=True), (16, B)))
        extra = jnp.where(
            sub < 3,
            1.0,
            jnp.where(sub == 3, hi, jnp.where(sub == 4, mid, jnp.where(sub == 5, low, 0.0))),
        )
        right_t[:B, at] = wide.astype(bf16)
        right_t[B : B + 16, at] = extra.astype(bf16)
        right_t[B + 16 :, at] = jnp.zeros((B - 16, B), bf16)

    places = []
    for a in range(16):
        dx, dy = (a // 4 - x + 4) % 4, (a // 2 % 2 - y_hi + 2) % 2
        k = jnp.int32(0)
        for i, d in enumerate(PLANE):
            k = jnp.where((dx == d[0]) & (dy == d[1]), i, k)
        places.append(pl.multiple_of((2 * k + (a % 2 - core + 2) % 2) * B, B))

    def relayout(s):
        wait_for("tile", s)

        def group(g, carry):
            at = pl.ds(pl.multiple_of(s * B + g * 16, 16), 16)
            turned = pltpu.einshape("iap->aip", tile[at])
            for a in range(16):
                flat[at, pl.ds(places[a], B)] = turned[a]
            return carry

        lax.fori_loop(0, B // 16, group, 0, unroll=2)

    def arrive_z(d):
        wait_for("z", d)
        start(to_y[d])

    def arrive_plane(k):
        wait_for("plane", k)
        start(to_core[k])

    with jax.named_scope("relayout"):
        prepare_col(0)
        prepare_row(own)
        for s in range(EARLY):
            relayout(s)
    arrive_plane(ACROSS)
    for k in (7, 6, 5):
        start(to_plane[k])
    for k in (1, 2, 3):
        arrive_plane(k)
    for d in (1, -1):
        arrive_z(d)
    for d in (2, -2):
        arrive_z(d)
    for d in (4, 3, -3):
        start(to_z[d])
    with jax.named_scope("relayout2"):
        for s in range(EARLY, 16):
            relayout(s)
    for k in range(1, NEAR):
        prepare_col(2 * k)
    def from_core(chips):
        wait_for("core", chips[0])
        for k in chips:
            prepare_col(2 * k + 1)

    from_core(range(NEAR))

    def f_place(g):
        d, h = g
        return at_y if d == 0 or h and d in FAR else at_z(d)

    def f_from(g):
        d, h = g
        return g if h and d in FAR or d in (0, 4) else (-d, h)

    def f_slot(g):
        d, h = g
        return POS[d % 8, 1] if h and d in FAR else POS[-d % 8, h]

    f_sends = {
        g: remote(f_out.at[POS[g[0] % 8, g[1]]], f_in.at[f_slot(g)], sem("f", f_from(g)), f_place(g))
        for g in GROUPS
        if g != (0, 0)
    }
    d_sends = {k: remote(d_out.at[k], d_in.at[k], sem("d", k), at_core) for k in range(8)}
    p_sends = {
        k: remote(
            p_out.at[k],
            p_in.at[opposite(k)],
            sem("p", opposite(k)),
            at_plane(k),
        )
        for k in range(1, 8)
    }
    def first_terms(s):
        both = prods[pl.ds(s * B, B), :]
        return both[:, B:] * left[pl.ds(s * B, B), :B].astype(f32) - both[:, :B]

    def arrived(g):
        wait_for("f", g)
        return f_in[POS[g[0] % 8, g[1]]].astype(f32)

    def give_first(g):
        s = POS[g[0] % 8, g[1]]
        terms = first_terms(s)
        if g == (0, 1):
            for d in (1, -1, 2, -2):
                terms += arrived((d, 1))
        if g[0] in FAR and g[1] == 0:
            terms += arrived((g[0], 1))
        f_out[s] = terms.astype(bf16)
        pending.append(f_sends[g])

    def second_terms(a):
        at = pl.ds(a * B, B)
        return second_t[B : B + 1, at] * right_t[:B, at].astype(f32) - second_t[:B, at]

    def weigh(rows, cs):
        power = jnp.dot(left[rows, :], right_t[:, cs], preferred_element_type=f32)
        return (flat[rows, cs].astype(f32) * jnp.exp(power)).astype(bf16)

    def make_weights(u):
        first, n, low, high = UNITS[u]
        rows = pl.ds(first * B, n * B)
        for c in range(low, high):
            cs = slice(c * 2 * B, (c + 1) * 2 * B)
            weights[u % 2, : n * B, cs] = weigh(rows, cs)

    seen_rows, seen_cols = set(), set()

    def use_weights(u):
        first, n, low, high = UNITS[u]
        rows, cs = pl.ds(first * B, n * B), slice(low * 2 * B, high * 2 * B)
        held = weights[u % 2, : n * B, cs]
        for i in range(0, n, 2):
            part = jnp.dot(held[i * B : (i + 2) * B], right[cs, :], preferred_element_type=f32)
            to = pl.ds((first + i) * B, 2 * B)
            if first + i in seen_rows:
                prods[to, :] += part
            else:
                prods[to, :] = part
            seen_rows.add(first + i)
        term = jnp.dot(left_t[:, rows], held, preferred_element_type=f32)
        if low in seen_cols:
            second_t[:, cs] += term
        else:
            second_t[:, cs] = term
        seen_cols.update(range(low, high))

    done = {GROUPS[i]: u + 1 for u, (first, n, _, _) in enumerate(UNITS) for i in range(first, first + n)}
    def need(g):
        d, h = g
        if g == (0, 0):
            return
        if h == 1:
            wait_for("y", d)

    pending = []

    def flush():
        while pending:
            start(pending.pop(0))

    def give_core(k):
        d_out[k] = second_terms(2 * k + 1).astype(bf16)
        pending.append(d_sends[k])

    def give_plane(k):
        wait_for("d", k)
        terms = second_terms(2 * k) + d_in[k].astype(f32)
        p_out[k] = terms.astype(bf16)
        pending.append(p_sends[k])

    p_queue = [7, 6, 5, 4, 3, 2, 1]
    core_done = {}
    ready = {(0, 0)}

    def fresh(u):
        return [g for g in GROUPS[UNITS[u][0] : UNITS[u][0] + UNITS[u][1]] if g not in ready]

    for g in fresh(0):
        need(g)
        prepare_row(POS[g[0] % 8, g[1]])
        ready.add(g)
    for t in range(len(UNITS) + 1):
        flush()
        if t == 2:
            arrive_plane(6)
            arrive_plane(5)
            arrive_plane(7)
        if t == 4:
            from_core(range(NEAR, 8))
        if t == 3:
            for k in range(NEAR, 8):
                prepare_col(2 * k)
        nexts = []
        for u in (t, t + 1):
            if u < len(UNITS) and (u == t or u not in LATE):
                for g in fresh(u):
                    need(g)
                    ready.add(g)
                    if u == t:
                        prepare_row(POS[g[0] % 8, g[1]])
                    else:
                        nexts.append(g)
        if t in EXTRA:
            nexts.append(EXTRA[t])
            ready.add(EXTRA[t])
        if t == 2:
            for d in (4, 3, -3):
                arrive_z(d)
        if t < len(UNITS):
            make_weights(t)
        for g in nexts:
            prepare_row(POS[g[0] % 8, g[1]])
        if t > 0:
            use_weights(t - 1)
        if t > 0 and UNITS[t - 1][0] == 2 * len(PAIRS):
            for k in reversed(range(*UNITS[t - 1][2:])):
                give_core(k)
                core_done[k] = t
        for g in GROUPS:
            if done[g] == t and t < len(UNITS) and g not in ((0, 1), (4, 0)):
                give_first(g)
        while p_queue and core_done.get(p_queue[0], t) + NEXT_P <= t:
            give_plane(p_queue.pop(0))
    flush()
    while p_queue and p_queue[0] > 3:
        give_plane(p_queue.pop(0))
        if len(pending) > 1:
            start(pending.pop(0))
    for g in ((4, 0), (3, 0), (-3, 0)):
        give_first(g)
        if len(pending) > 1:
            start(pending.pop(0))
    while p_queue and p_queue[0] > 1:
        give_plane(p_queue.pop(0))
        start(pending.pop(0))
    give_first((-1, 0))
    start(pending.pop(0))
    give_plane(1)
    flush()
    mine_t = second_terms(0) + d_in[0].astype(f32)
    mine = first_terms(own)
    flush()
    give_first((0, 1))
    flush()
    for k in reversed(range(1, 8)):
        wait_for("p", k)
        mine_t += p_in[k].astype(f32)
    mine += mine_t.T
    for g in ((2, 0), (-2, 0), (1, 0), (-1, 0), (0, 1), (3, 0), (-3, 0), (4, 0)):
        mine += arrived(g)
    out[...] = mine
    all_sent = flat.at[pl.ds(0, len(n_sent) * B * B // N)]
    with jax.named_scope("sent"):
        pltpu.make_async_copy(all_sent, all_sent, sent).wait()


def per_device(points, abar, inv_scale):
    vmem, dma = pltpu.VMEM, pltpu.SemaphoreType.DMA
    blocks = lambda n: vmem((n, B, B), bf16)
    total = pl.pallas_call(
        kernel,
        out_shape=jax.ShapeDtypeStruct((B, B), f32),
        in_specs=[pl.BlockSpec(memory_space=pltpu.HBM)] * 3,
        out_specs=pl.BlockSpec(memory_space=vmem),
        scratch_shapes=[
            blocks(16), blocks(16), vmem((1, B), f32),
            vmem((N, 16, B), bf16), vmem((N, N), bf16),
            vmem((N, 2 * B), bf16), vmem((2 * B, N), bf16), vmem((N, 2 * B), bf16), vmem((B + 16, N), bf16),
            vmem((2, 4 * B, N), bf16), vmem((N, 2 * B), f32), vmem((B + 16, N), f32),
            blocks(16), blocks(16), *[blocks(8) for _ in range(4)],
            dma((len(COPIES),)), dma,
        ],
        compiler_params=pltpu.CompilerParams(
            collective_id=0, has_side_effects=True, vmem_limit_bytes=40 * 2**20
        ),
    )(*[pltpu.with_memory_space_constraint(v, pltpu.HBM) for v in (points, abar.reshape(N, 16, B), inv_scale.reshape(1, B))])
    return -total * inv_scale[None, :]


def solution(mesh):
    placed = (P(("row", "col"), None), P("row", None, "col", None), P())
    return jax.shard_map(
        per_device, mesh=mesh, in_specs=placed, out_specs=P(("row", "col"), None), check_vma=False
    )
```
